32 devices in a mesh: gx: 4 (over y, x), gy: 4 (over z), row: 2 (over core).
Axes of the slice: x: 2, y: 2, z: 4, core: 2. Of those that a mesh axis runs over, the one named last changes fastest.
Arguments:
- columns: bfloat16 [137, 131072], P(None, ('gx', 'gy')), may hold values from -6 to 6
- level_weights: bfloat16 [137, 16], replicated, may hold values from -0.5 to 0.5
- orbit_term: float32 [16, 32], replicated, may hold values from -6 to 6
- col_owner: int32 [524288, 1], P(('gx', 'gy', 'row')), may hold values from 0 to 15; in each aligned block of 16384 rows (0 to 16383, 16384 to 32767, ...) at most 2048 rows name the same one
- col_local: int32 [524288], P(('gx', 'gy', 'row')), may hold values from 0 to 8191
- orbit_bin: int32 [524288], P(('gx', 'gy', 'row')), may hold values from 0 to 31
- group_id: int32 [524288], P(('gx', 'gy', 'row')), may hold values from 0 to 63
- departure: float32 [524288], P(('gx', 'gy', 'row')), may hold values from -6 to 6
Outputs:
- covariance: float32 [16, 16, 64], P(None, None, 'row')
- cross: float32 [16, 64], P(None, 'row')
The draws below stay inside these ranges and needn't reach their ends.
Inputs may be any that keep to these rules, and one draw needn't show every extreme that they name: `col_owner`: among the footprints of one device, no owning device is named more than 2048 times; some owning device is named exactly 2048 times.
All inputs are finite; a program needn't handle non-finite values.
Results may differ from the reference program's by a relative error of at most 0.0022.
Values may be sent and summed in bfloat16 or wider, within the bound.
A program may use at most 128 MiB of HBM per device.

```python
import math
import jax
import jax.numpy as jnp
import numpy as np
from jax import lax

L = 137
NP = 16
NGRP = 64
NBIN = 32
C_DEV = 8192
FP_DEV = 16384
CAP = 2048
NCOL = 131072
NFP = 524288
N_GX = 4
N_GY = 4
DEVICES = 32


def touch_ends(values, stream_key, least, top_value):
    extent = values.shape
    index_at = [jax.random.randint(jax.random.fold_in(stream_key, axis), (), 0, extent[axis]) for axis in range(len(extent))]
    values = values.at[tuple(index_at)].set(least)
    longest = extent.index(max(extent))
    index_at[longest] = (index_at[longest] + 1) % extent[longest]
    return values.at[tuple(index_at)].set(top_value)


def block_levels(rng, shape, split, smallest, high):
    loudness = 1.0
    for position, blocks in split:
        draws = jax.random.uniform(jax.random.fold_in(jax.random.fold_in(rng, 6), position), (blocks,), jnp.float32, smallest / len(split), high / len(split))
        loudness = loudness * jnp.repeat(jnp.exp(draws), shape[position] // blocks).reshape((-1,) + (1,) * (len(shape) - 1 - position))
    return loudness


def deal_out(rng, own, number, rows, amount, top, reach, slope):
    sequence = jax.random.permutation(rng, amount)
    heavy_load, common = load_shares(amount, rows * top, reach, slope, True), load_shares(amount, rows * top, reach, slope, False)
    places = jnp.arange(amount)

    def named(tallies, turn):
        used = int((tallies > 0).sum())
        fixed = max(1, used // 4)
        moved = fixed + (places - fixed + turn * (used - fixed)) % max(1, amount - fixed)
        return jnp.zeros((amount,), jnp.int32).at[sequence[jnp.where(places < fixed, places, moved)]].set(jnp.asarray(tallies, jnp.int32))

    tallies = jnp.where(number % 4 == 0, named(heavy_load, number // 4), named(common, number - number // 4 - 1))
    mixed = jax.random.permutation(jax.random.fold_in(own, 3), amount)
    source_of, sink = mixed[0:amount // 2 * 2:2], mixed[1:amount // 2 * 2:2]
    room = jnp.minimum(tallies[source_of] - 1, reach - tallies[sink]) // 2
    room = jnp.where((source_of == sequence[0]) | (sink == sequence[0]) | (tallies[sink] == 0), 0, jnp.maximum(room, 0))
    moved = jax.random.randint(jax.random.fold_in(own, 4), (amount // 2,), 0, 1 << 20) % (room + 1)
    tallies = tallies.at[source_of].add(-moved).at[sink].add(moved)
    labels = jnp.searchsorted(jnp.cumsum(tallies), jnp.arange(rows * top), side="right").astype(jnp.int32)
    table = labels.reshape(top, rows).T
    table = table[jax.random.permutation(jax.random.fold_in(own, 1), rows)]
    turn = jax.random.randint(jax.random.fold_in(own, 2), (rows, 1), 0, top)
    return jnp.take_along_axis(table, (jnp.arange(top)[None, :] + turn) % top, axis=1)


def load_shares(number_of, total, reach, slope, full):
    weights = [(1 << 20) // math.isqrt(standing ** slope) + 1 for standing in range(1, number_of + 1)]
    largest = reach if full else min(reach, max(-(-total // number_of), total * weights[0] // sum(weights)))
    least = 1 if total - largest >= number_of - 1 else 0
    counts, surplus = [largest] + [least] * (number_of - 1), total - largest - least * (number_of - 1)
    while surplus > 0:
        free = [i for i in range(1, number_of) if counts[i] < largest] or [i for i in range(1, number_of) if counts[i] < reach]
        pool, left = sum([weights[i] for i in free]), surplus
        for i in free:
            addition = min(reach - counts[i], max(1, left * weights[i] // pool), surplus)
            counts[i] = counts[i] + addition
            surplus = surplus - addition
    return np.array(counts)


def bell_draw(stream_key, shape, scale, most, cuts=(), kind=jnp.bfloat16):
    loudness = block_levels(stream_key, shape, cuts, -0.22, 0.18) if cuts else 1.0
    values = jax.random.normal(stream_key, shape, jnp.float32) * scale * loudness
    return jnp.minimum(jnp.maximum(values, -most), most).astype(kind)


def setup_inputs(seed: int = 0) -> dict:
    key_list = jax.random.split(jax.random.key(seed), 9)
    columns = bell_draw(key_list[0], (L, NCOL), 1.0, 6.0, ((1, 16),))
    level_weights = bell_draw(key_list[1], (L, NP), L ** -0.5, 0.5)
    orbit_term = bell_draw(key_list[2], (NP, NBIN), 1.0, 6.0, (), jnp.float32)
    col_owner_keys = jax.random.split(jax.random.fold_in(key_list[3], 1), NFP // FP_DEV)
    col_owner_turns = jax.random.permutation(jax.random.fold_in(key_list[3], 3), NFP // FP_DEV)
    col_owner = jax.vmap(lambda own, number: deal_out(jax.random.fold_in(key_list[3], 2), own, number, FP_DEV, N_GX * N_GY, 1, CAP, 1))(col_owner_keys, col_owner_turns).reshape((NFP, 1))
    col_local = touch_ends(jax.random.randint(key_list[4], (NFP,), 0, C_DEV), jax.random.fold_in(key_list[4], 1), 0, C_DEV - 1).astype(jnp.int32)
    orbit_bin = touch_ends(jax.random.randint(key_list[5], (NFP,), 0, NBIN), jax.random.fold_in(key_list[5], 1), 0, NBIN - 1).astype(jnp.int32)
    group_id = touch_ends(jax.random.randint(key_list[6], (NFP,), 0, NGRP), jax.random.fold_in(key_list[6], 1), 0, NGRP - 1).astype(jnp.int32)
    departure = bell_draw(key_list[7], (NFP,), 1.0, 6.0, ((0, 32),), jnp.float32)
    return dict(columns=columns, level_weights=level_weights, orbit_term=orbit_term, col_owner=col_owner, col_local=col_local, orbit_bin=orbit_bin, group_id=group_id, departure=departure)


def reference(columns, level_weights, orbit_term, col_owner, col_local, orbit_bin, group_id, departure):
    thickness = jnp.dot(level_weights.T, columns, preferred_element_type=jnp.float32).astype(jnp.bfloat16)
    index = (col_owner[:, 0].astype(jnp.int32) * C_DEV + col_local.astype(jnp.int32)).astype(jnp.int32)
    predictors = thickness[:, index].astype(jnp.float32) + orbit_term[:, orbit_bin]
    blocks = predictors.reshape(NP, DEVICES, FP_DEV).transpose(1, 0, 2)
    groups = group_id.reshape(DEVICES, FP_DEV)
    depart = departure.reshape(DEVICES, FP_DEV)

    def accumulate(carry, parts):
        prod_acc, sum_acc, count_acc = carry
        block, grp, dep = parts
        outer = (block[:, None, :] * block[None, :, :]).reshape(NP * NP, -1)
        prod_acc = prod_acc + jax.ops.segment_sum(outer.T, grp, NGRP).T
        sum_acc = sum_acc + jax.ops.segment_sum((block * dep[None, :]).T, grp, NGRP).T
        count_acc = count_acc + jax.ops.segment_sum(jnp.ones_like(dep), grp, NGRP)
        return (prod_acc, sum_acc, count_acc), None

    start = (jnp.zeros((NP * NP, NGRP), jnp.float32), jnp.zeros((NP, NGRP), jnp.float32), jnp.zeros((NGRP,), jnp.float32))
    (products, sums, count), _ = lax.scan(accumulate, start, (blocks, groups, depart))
    scale = 1.0 / (count + 1.0)
    covariance = (products * scale[None, :]).reshape(NP, NP, NGRP)
    cross = sums * scale[None, :]
    return covariance, cross
```

```python
import math

import jax
import jax.numpy as jnp
from jax import lax
from jax.experimental import pallas as pl
from jax.experimental.pallas import tpu as pltpu
from jax.sharding import PartitionSpec as P

NGRP = 64
LANES = 128
CHUNK = 256
TABLE_LIMIT = 24 * 1024 * 1024
AXES = ("gx", "gy", "row")


def send_request(wanted):
    return lax.all_to_all(wanted, ("gx", "gy"), split_axis=0, concat_axis=0, tiled=True)


def send_answer(picked):
    return lax.all_to_all(picked, ("gx", "gy"), split_axis=1, concat_axis=1, tiled=True)


def routed(columns, level_weights, orbit_term, col_owner, col_local, orbit_bin, group_id, departure):
    grid_x = lax.axis_size("gx")
    grid_y = lax.axis_size("gy")
    owners = grid_x * grid_y
    footprints = col_owner.shape[0]
    capacity = 2 * footprints // owners
    slots_all = owners * capacity
    npred = level_weights.shape[1]
    ngroups = NGRP
    owner = col_owner[:, 0]
    owner_hits = (owner[:, None] == jnp.arange(owners, dtype=jnp.int32)[None, :]).astype(jnp.int32)
    ranks = jnp.cumsum(owner_hits, axis=0)
    slot = jnp.sum(ranks * owner_hits, axis=1) - 1
    target = owner * capacity + slot
    stacked = jnp.stack([col_local, orbit_bin, group_id], axis=0)
    placed = jnp.full((3, slots_all), -1, jnp.int32).at[:, target].set(stacked)
    slot_depart = jnp.zeros((slots_all,), jnp.float32).at[target].set(departure)
    wanted = jnp.maximum(placed[0], 0).reshape(owners, capacity)
    asked = send_request(wanted)
    thickness = jnp.dot(level_weights.T, columns, preferred_element_type=jnp.float32).astype(
        jnp.bfloat16
    )
    picked = thickness[:, asked]
    back = send_answer(picked)
    flat = back.reshape(npred, slots_all)
    slot_bin = placed[1]
    slot_group = placed[2]
    width = math.gcd(slots_all, 4096)
    nblocks = slots_all // width
    bin_range = jnp.arange(orbit_term.shape[1], dtype=jnp.int32)
    group_range = jnp.arange(ngroups, dtype=jnp.int32)

    def accumulate(carry, which):
        prod_acc, sum_acc, count_acc = carry
        first = which * width
        part_flat = lax.dynamic_slice_in_dim(flat, first, width, 1)
        part_bin = lax.dynamic_slice_in_dim(slot_bin, first, width, 0)
        grp = lax.dynamic_slice_in_dim(slot_group, first, width, 0)
        dep = lax.dynamic_slice_in_dim(slot_depart, first, width, 0)
        bin_hits = (bin_range[:, None] == part_bin[None, :]).astype(jnp.float32)
        block = part_flat.astype(jnp.float32) + jnp.dot(
            orbit_term,
            bin_hits,
            precision=lax.Precision.HIGHEST,
            preferred_element_type=jnp.float32,
        )
        hits = (grp[:, None] == group_range[None, :]).astype(jnp.float32)
        outer = (block[:, None, :] * block[None, :, :]).reshape(npred * npred, width)
        prod_acc = prod_acc + jnp.dot(
            outer, hits, precision=lax.Precision.HIGHEST, preferred_element_type=jnp.float32
        )
        sum_acc = sum_acc + jnp.dot(
            block * dep[None, :],
            hits,
            precision=lax.Precision.HIGHEST,
            preferred_element_type=jnp.float32,
        )
        count_acc = count_acc + jnp.sum(hits, axis=0)[None, :]
        return ((prod_acc, sum_acc, count_acc), None)

    start = (
        jnp.zeros((npred * npred, ngroups), jnp.float32),
        jnp.zeros((npred, ngroups), jnp.float32),
        jnp.zeros((1, ngroups), jnp.float32),
    )
    (products, sums, count), _ = lax.scan(accumulate, start, jnp.arange(nblocks, dtype=jnp.int32))
    share = ngroups // lax.axis_size("row")
    products, sums, count = (
        lax.psum_scatter(products, "row", scatter_dimension=1, tiled=True),
        lax.psum_scatter(sums, "row", scatter_dimension=1, tiled=True),
        lax.psum_scatter(count, "row", scatter_dimension=1, tiled=True),
    )
    products, sums, count = lax.psum((products, sums, count), ("gx", "gy"))
    scale = 1.0 / (count + 1.0)
    covariance = (products * scale).reshape(npred, npred, share)
    cross = sums * scale
    return (covariance, cross)


def table_kernel(weights_ref, columns_ref, out_ref, *, npred, stripes):
    rows = out_ref.shape[0]
    weights = weights_ref[...]
    parts = []
    for s in range(stripes):
        cols = columns_ref[:, s * rows:(s + 1) * rows]
        parts.append(
            lax.dot_general(weights, cols, (((0,), (0,)), ((), ())), preferred_element_type=jnp.float32)
        )
    out_ref[...] = jnp.concatenate(parts, axis=0).T.astype(jnp.bfloat16)


def stats_kernel(index_ref, table_ref, packed_ref, depart_ref, orbit_ref, out_ref, wide_ref, even_ref, odd_ref,
                 *, npred, stripes, sbits, bbits):
    rows = table_ref.shape[0]
    step = 512

    def widen(i, carry):
        at = pl.multiple_of(i * step, step)
        wide_ref[pl.ds(at, step), :] = table_ref[pl.ds(at, step), :].astype(jnp.float32)
        return carry

    lax.fori_loop(0, rows // step, widen, 0)
    nchunks = packed_ref.shape[0]

    def pull(chunk, into):
        first = chunk * CHUNK
        for i in range(CHUNK):
            into[i:i + 1, :] = wide_ref[pl.ds(index_ref[first + i], 1), :]

    def fold(chunk, held):
        packed = packed_ref[pl.ds(chunk, 1), :]
        dep = depart_ref[pl.ds(chunk, 1), :]
        stripe = packed & (stripes - 1)
        obin = (packed >> sbits) & ((1 << bbits) - 1)
        grp = packed >> (sbits + bbits)
        turned = held[...].T
        stripe = jnp.broadcast_to(stripe, (npred, CHUNK))
        pred = turned[0:npred]
        for s in range(1, stripes):
            pred = jnp.where(stripe == s, turned[s * npred:(s + 1) * npred], pred)
        orbit = orbit_ref[...]
        obin = jnp.broadcast_to(obin, (npred, CHUNK))
        terms = [
            jnp.take_along_axis(orbit, obin[:, a:a + LANES], axis=1, mode="promise_in_bounds")
            for a in range(0, CHUNK, LANES)
        ]
        pred = pred + jnp.concatenate(terms, axis=1)
        hits = (lax.broadcasted_iota(jnp.int32, (NGRP, CHUNK), 0) == grp).astype(jnp.float32).astype(jnp.bfloat16)
        pieces = [pred[i:i + 1, :] * pred for i in range(npred)]
        pieces.append(pred * dep)
        pieces.append(jnp.ones((16, CHUNK), jnp.float32))
        full = jnp.concatenate(pieces, axis=0)
        high = full.astype(jnp.bfloat16)
        low = (full - high.astype(jnp.float32)).astype(jnp.bfloat16)
        dims = (((1,), (1,)), ((), ()))
        return lax.dot_general(high, hits, dims, preferred_element_type=jnp.float32) + lax.dot_general(
            low, hits, dims, preferred_element_type=jnp.float32
        )

    out_ref[...] = jnp.zeros_like(out_ref)
    pull(0, even_ref)

    def pair(j, carry):
        pull(2 * j + 1, odd_ref)
        out_ref[...] += fold(2 * j, even_ref)
        pull(jnp.minimum(2 * j + 2, nchunks - 1), even_ref)
        out_ref[...] += fold(2 * j + 1, odd_ref)
        return carry

    lax.fori_loop(0, nchunks // 2, pair, 0)


def local(columns, level_weights, orbit_term, col_owner, col_local, orbit_bin, group_id, departure):
    owners = lax.axis_size("gx") * lax.axis_size("gy")
    nrow = lax.axis_size("row")
    levels, cdev = columns.shape
    npred = level_weights.shape[1]
    nbin = orbit_term.shape[1]
    stripes = LANES // npred
    half = cdev // nrow
    rows = half // stripes
    total = owners * nrow * rows
    if total * LANES * 4 > TABLE_LIMIT:
        return routed(
            columns, level_weights, orbit_term, col_owner, col_local, orbit_bin, group_id, departure
        )
    footprints = col_local.shape[0]
    nchunks = footprints // CHUNK
    sbits = (stripes - 1).bit_length()
    bbits = (nbin - 1).bit_length()

    mine = lax.dynamic_slice_in_dim(columns, lax.axis_index("row") * half, half, 1)
    piece = pl.pallas_call(
        lambda *refs: table_kernel(*refs, npred=npred, stripes=stripes),
        out_shape=jax.ShapeDtypeStruct((rows, LANES), jnp.bfloat16),
        name="table",
    )(level_weights, mine)
    table = lax.all_gather(piece, AXES, axis=0, tiled=True)

    index = (col_owner[:, 0] * nrow + col_local // half) * rows + col_local % rows
    stripe = (col_local % half) // rows
    packed = stripe | (orbit_bin << sbits) | (group_id << (sbits + bbits))
    orbit = jnp.pad(orbit_term, ((0, 0), (0, LANES - nbin)))
    vmem = pl.BlockSpec(memory_space=pltpu.VMEM)
    height = npred * npred + npred + 16
    stats = pl.pallas_call(
        lambda *refs: stats_kernel(*refs, npred=npred, stripes=stripes, sbits=sbits, bbits=bbits),
        out_shape=jax.ShapeDtypeStruct((height, NGRP), jnp.float32),
        in_specs=[pl.BlockSpec(memory_space=pltpu.SMEM), vmem, vmem, vmem, vmem],
        out_specs=vmem,
        scratch_shapes=[
            pltpu.VMEM((total, LANES), jnp.float32),
            pltpu.VMEM((CHUNK, LANES), jnp.float32),
            pltpu.VMEM((CHUNK, LANES), jnp.float32),
        ],
        compiler_params=pltpu.CompilerParams(vmem_limit_bytes=40 * 1024 * 1024),
        name="stats",
    )(index, table, packed.reshape(nchunks, CHUNK), departure.reshape(nchunks, CHUNK), orbit)

    share = NGRP // nrow
    stats = lax.psum_scatter(stats, "row", scatter_dimension=1, tiled=True)
    stats = lax.psum(stats, ("gx", "gy"))
    square = npred * npred
    scale = 1.0 / (stats[square + npred:square + npred + 1] + 1.0)
    covariance = (stats[:square] * scale).reshape(npred, npred, share)
    cross = stats[square:square + npred] * scale
    return (covariance, cross)


def solution(mesh):
    in_specs = (
        P(None, ("gx", "gy")),
        P(),
        P(),
        P(("gx", "gy", "row"), None),
        P(("gx", "gy", "row")),
        P(("gx", "gy", "row")),
        P(("gx", "gy", "row")),
        P(("gx", "gy", "row")),
    )
    out_specs = (P(None, None, "row"), P(None, "row"))
    return jax.shard_map(local, mesh=mesh, in_specs=in_specs, out_specs=out_specs, check_vma=False)
```

```python
import math

import jax
import jax.numpy as jnp
from jax import lax
from jax.experimental import pallas as pl
from jax.experimental.pallas import tpu as pltpu
from jax.sharding import PartitionSpec as P

NGRP = 64
LANES = 128
CHUNK = 256
TABLE_LIMIT = 24 * 1024 * 1024
AXES = ("gx", "gy", "row")


def send_request(wanted):
    return lax.all_to_all(wanted, ("gx", "gy"), split_axis=0, concat_axis=0, tiled=True)


def send_answer(picked):
    return lax.all_to_all(picked, ("gx", "gy"), split_axis=1, concat_axis=1, tiled=True)


def routed(columns, level_weights, orbit_term, col_owner, col_local, orbit_bin, group_id, departure):
    grid_x = lax.axis_size("gx")
    grid_y = lax.axis_size("gy")
    owners = grid_x * grid_y
    footprints = col_owner.shape[0]
    capacity = 2 * footprints // owners
    slots_all = owners * capacity
    npred = level_weights.shape[1]
    ngroups = NGRP
    owner = col_owner[:, 0]
    owner_hits = (owner[:, None] == jnp.arange(owners, dtype=jnp.int32)[None, :]).astype(jnp.int32)
    ranks = jnp.cumsum(owner_hits, axis=0)
    slot = jnp.sum(ranks * owner_hits, axis=1) - 1
    target = owner * capacity + slot
    stacked = jnp.stack([col_local, orbit_bin, group_id], axis=0)
    placed = jnp.full((3, slots_all), -1, jnp.int32).at[:, target].set(stacked)
    slot_depart = jnp.zeros((slots_all,), jnp.float32).at[target].set(departure)
    wanted = jnp.maximum(placed[0], 0).reshape(owners, capacity)
    asked = send_request(wanted)
    thickness = jnp.dot(level_weights.T, columns, preferred_element_type=jnp.float32).astype(
        jnp.bfloat16
    )
    picked = thickness[:, asked]
    back = send_answer(picked)
    flat = back.reshape(npred, slots_all)
    slot_bin = placed[1]
    slot_group = placed[2]
    width = math.gcd(slots_all, 4096)
    nblocks = slots_all // width
    bin_range = jnp.arange(orbit_term.shape[1], dtype=jnp.int32)
    group_range = jnp.arange(ngroups, dtype=jnp.int32)

    def accumulate(carry, which):
        prod_acc, sum_acc, count_acc = carry
        first = which * width
        part_flat = lax.dynamic_slice_in_dim(flat, first, width, 1)
        part_bin = lax.dynamic_slice_in_dim(slot_bin, first, width, 0)
        grp = lax.dynamic_slice_in_dim(slot_group, first, width, 0)
        dep = lax.dynamic_slice_in_dim(slot_depart, first, width, 0)
        bin_hits = (bin_range[:, None] == part_bin[None, :]).astype(jnp.float32)
        block = part_flat.astype(jnp.float32) + jnp.dot(
            orbit_term,
            bin_hits,
            precision=lax.Precision.HIGHEST,
            preferred_element_type=jnp.float32,
        )
        hits = (grp[:, None] == group_range[None, :]).astype(jnp.float32)
        outer = (block[:, None, :] * block[None, :, :]).reshape(npred * npred, width)
        prod_acc = prod_acc + jnp.dot(
            outer, hits, precision=lax.Precision.HIGHEST, preferred_element_type=jnp.float32
        )
        sum_acc = sum_acc + jnp.dot(
            block * dep[None, :],
            hits,
            precision=lax.Precision.HIGHEST,
            preferred_element_type=jnp.float32,
        )
        count_acc = count_acc + jnp.sum(hits, axis=0)[None, :]
        return ((prod_acc, sum_acc, count_acc), None)

    start = (
        jnp.zeros((npred * npred, ngroups), jnp.float32),
        jnp.zeros((npred, ngroups), jnp.float32),
        jnp.zeros((1, ngroups), jnp.float32),
    )
    (products, sums, count), _ = lax.scan(accumulate, start, jnp.arange(nblocks, dtype=jnp.int32))
    share = ngroups // lax.axis_size("row")
    products, sums, count = (
        lax.psum_scatter(products, "row", scatter_dimension=1, tiled=True),
        lax.psum_scatter(sums, "row", scatter_dimension=1, tiled=True),
        lax.psum_scatter(count, "row", scatter_dimension=1, tiled=True),
    )
    products, sums, count = lax.psum((products, sums, count), ("gx", "gy"))
    scale = 1.0 / (count + 1.0)
    covariance = (products * scale).reshape(npred, npred, share)
    cross = sums * scale
    return (covariance, cross)


def grid_place(gx, gy, row, n_gy, n_row):
    return (gx * n_gy + gy) * n_row + row


def table_kernel(weights_ref, columns_ref, out_ref, send_sems, recv_sems, *, npred, stripes, n_gy, n_row):
    rows = columns_ref.shape[1] // stripes
    gx, gy, row = lax.axis_index("gx"), lax.axis_index("gy"), lax.axis_index("row")
    low_bit, high_bit = gx % 2, gx // 2
    low_step, high_step = 1 - 2 * low_bit, 2 * (1 - 2 * high_bit)
    gx_a = gx + (1 - row) * low_step + row * high_step
    gx_b = gx + row * low_step + (1 - row) * high_step
    gx_ab = gx + low_step + high_step
    gys = [(gy + i) % n_gy for i in range(n_gy)]
    along = [(gx, gys[i], row) for i in range(1, n_gy)]
    to_a, to_b, mate = (gx_a, gy, row), (gx_b, gy, row), (gx, gy, 1 - row)
    peers = along + [to_a, to_b, mate]

    barrier = pltpu.get_barrier_semaphore()
    for peer in peers:
        pl.semaphore_signal(barrier, inc=1, device_id=peer, device_id_type=pl.DeviceIdType.MESH)

    weights = weights_ref[...]
    parts = []
    for s in range(stripes):
        cols = columns_ref[:, s * rows:(s + 1) * rows]
        parts.append(
            lax.dot_general(weights, cols, (((0,), (0,)), ((), ())), preferred_element_type=jnp.float32)
        )
    own = grid_place(gx, gy, row, n_gy, n_row)
    out_ref[pl.ds(pl.multiple_of(own * rows, rows), rows), :] = (
        jnp.concatenate(parts, axis=0).T.astype(jnp.bfloat16)
    )
    pl.semaphore_wait(barrier, len(peers))

    sent = []

    def copy(block, peer, number):
        at = out_ref.at[pl.ds(pl.multiple_of(block * rows, rows), rows), :]
        return pltpu.make_async_remote_copy(
            src_ref=at, dst_ref=at, send_sem=send_sems.at[number], recv_sem=recv_sems.at[block],
            device_id=peer, device_id_type=pl.DeviceIdType.MESH,
        )

    def send(block, targets):
        for peer in targets:
            c = copy(block, peer, len(sent))
            c.start()
            sent.append(c)

    def arrive(block):
        copy(block, mate, 0).wait_recv()

    def place(x, y):
        return grid_place(x, y, row, n_gy, n_row)

    order = [0] + sorted(range(1, n_gy), key=lambda i: min(i, n_gy - i))
    send(own, along + [to_a, to_b, mate])
    arrive(place(gx_a, gy))
    send(place(gx_a, gy), [to_b, mate])
    arrive(place(gx_b, gy))
    send(place(gx_b, gy), [mate])
    for i in order[1:]:
        arrive(place(gx, gys[i]))
        send(place(gx, gys[i]), [to_a, to_b, mate])
    for i in order[1:]:
        arrive(place(gx_a, gys[i]))
        send(place(gx_a, gys[i]), [to_b, mate])
    arrive(place(gx_ab, gy))
    send(place(gx_ab, gy), [mate])
    for i in order[1:]:
        arrive(place(gx_b, gys[i]))
        send(place(gx_b, gys[i]), [mate])
        arrive(place(gx_ab, gys[i]))
        send(place(gx_ab, gys[i]), [mate])
    for x in (gx, gx_a, gx_b, gx_ab):
        for y in gys:
            arrive(grid_place(x, y, 1 - row, n_gy, n_row))
    for c in sent:
        c.wait_send()


def reduce_kernel(stats_ref, cov_ref, cross_ref, parts_ref, whole_ref, send_a, recv_a, send_b, recv_b,
                  *, npred, n_gx, n_gy, n_row, height):
    gx, gy, row = lax.axis_index("gx"), lax.axis_index("gy"), lax.axis_index("row")
    owners = n_gx * n_gy
    piece = whole_ref.shape[0] // owners
    mine = gx * n_gy + gy
    others = []
    for dx in range(n_gx):
        for dy in range(n_gy):
            for dr in range(n_row):
                if dx or dy or dr:
                    others.append(((gx + dx) % n_gx, (gy + dy) % n_gy, (row + dr) % n_row))
    barrier = pltpu.get_barrier_semaphore()
    for peer in others:
        pl.semaphore_signal(barrier, inc=1, device_id=peer, device_id_type=pl.DeviceIdType.MESH)
    pl.semaphore_wait(barrier, len(others))

    def rows_of(owner):
        return pl.ds(pl.multiple_of(owner * piece, piece), piece)

    me = mine * n_row + row
    first = []
    for k, peer in enumerate(others):
        owner = peer[0] * n_gy + peer[1]
        c = pltpu.make_async_remote_copy(
            src_ref=stats_ref.at[peer[2], rows_of(owner), :], dst_ref=parts_ref.at[me],
            send_sem=send_a.at[k], recv_sem=recv_a.at[me],
            device_id=peer, device_id_type=pl.DeviceIdType.MESH,
        )
        c.start()
        first.append(c)
    total = stats_ref[row, rows_of(mine), :]
    for k, peer in enumerate(others):
        who = grid_place(peer[0], peer[1], peer[2], n_gy, n_row)
        pltpu.make_async_remote_copy(
            src_ref=stats_ref.at[row, rows_of(mine), :], dst_ref=parts_ref.at[who],
            send_sem=send_a.at[k], recv_sem=recv_a.at[who],
            device_id=peer, device_id_type=pl.DeviceIdType.MESH,
        ).wait_recv()
        total = total + parts_ref[who]
    whole_ref[rows_of(mine), :] = total
    second = []
    for k, peer in enumerate(others):
        if k % n_row == n_row - 1:
            c = pltpu.make_async_remote_copy(
                src_ref=whole_ref.at[rows_of(mine), :], dst_ref=whole_ref.at[rows_of(mine), :],
                send_sem=send_b.at[len(second)], recv_sem=recv_b.at[mine],
                device_id=peer, device_id_type=pl.DeviceIdType.MESH,
            )
            c.start()
            second.append((c, peer))
    for k, (c, peer) in enumerate(second):
        owner = peer[0] * n_gy + peer[1]
        pltpu.make_async_remote_copy(
            src_ref=whole_ref.at[rows_of(owner), :], dst_ref=whole_ref.at[rows_of(owner), :],
            send_sem=send_b.at[k], recv_sem=recv_b.at[owner],
            device_id=peer, device_id_type=pl.DeviceIdType.MESH,
        ).wait_recv()
    share = cov_ref.shape[1]
    folds = LANES // share
    part = height // folds
    flat = jnp.concatenate([whole_ref[0:part, q * share:(q + 1) * share] for q in range(folds)], axis=0)
    square = npred * npred
    scale = 1.0 / (flat[square + npred:square + npred + 1] + 1.0)
    cov_ref[...] = flat[:square] * scale
    cross_ref[...] = flat[square:square + npred] * scale
    for c in first:
        c.wait_send()
    for c, _ in second:
        c.wait_send()


def stats_kernel(index_ref, table_ref, packed_ref, depart_ref, orbit_ref, out_ref, wide_ref, even_ref, odd_ref,
                 acc_ref, *, npred, stripes, sbits, bbits):
    rows = table_ref.shape[0]
    step = 512

    def widen(i, carry):
        at = pl.multiple_of(i * step, step)
        wide_ref[pl.ds(at, step), :] = table_ref[pl.ds(at, step), :].astype(jnp.float32)
        return carry

    lax.fori_loop(0, rows // step, widen, 0)
    nchunks = packed_ref.shape[0]

    def pull(chunk, into):
        first = chunk * CHUNK
        for i in range(CHUNK):
            into[i:i + 1, :] = wide_ref[pl.ds(index_ref[first + i], 1), :]

    def fold(chunk, held):
        packed = packed_ref[pl.ds(chunk, 1), :]
        dep = depart_ref[pl.ds(chunk, 1), :]
        stripe = packed & (stripes - 1)
        obin = (packed >> sbits) & ((1 << bbits) - 1)
        grp = packed >> (sbits + bbits)
        turned = held[...].T
        stripe = jnp.broadcast_to(stripe, (npred, CHUNK))
        pred = turned[0:npred]
        for s in range(1, stripes):
            pred = jnp.where(stripe == s, turned[s * npred:(s + 1) * npred], pred)
        orbit = orbit_ref[...]
        obin = jnp.broadcast_to(obin, (npred, CHUNK))
        terms = [
            jnp.take_along_axis(orbit, obin[:, a:a + LANES], axis=1, mode="promise_in_bounds")
            for a in range(0, CHUNK, LANES)
        ]
        pred = pred + jnp.concatenate(terms, axis=1)
        hits = (lax.broadcasted_iota(jnp.int32, (NGRP, CHUNK), 0) == grp).astype(jnp.float32).astype(jnp.bfloat16)
        pieces = [pred[i:i + 1, :] * pred for i in range(npred)]
        pieces.append(pred * dep)
        pieces.append(jnp.ones((16, CHUNK), jnp.float32))
        full = jnp.concatenate(pieces, axis=0)
        high = full.astype(jnp.bfloat16)
        low = (full - high.astype(jnp.float32)).astype(jnp.bfloat16)
        dims = (((1,), (1,)), ((), ()))
        return lax.dot_general(high, hits, dims, preferred_element_type=jnp.float32) + lax.dot_general(
            low, hits, dims, preferred_element_type=jnp.float32
        )

    acc_ref[...] = jnp.zeros_like(acc_ref)
    pull(0, even_ref)

    def pair(j, carry):
        pull(2 * j + 1, odd_ref)
        acc_ref[...] += fold(2 * j, even_ref)
        pull(jnp.minimum(2 * j + 2, nchunks - 1), even_ref)
        acc_ref[...] += fold(2 * j + 1, odd_ref)
        return carry

    lax.fori_loop(0, nchunks // 2, pair, 0)
    halves = out_ref.shape[0]
    share = NGRP // halves
    folds = LANES // share
    part = acc_ref.shape[0] // folds
    out_ref[...] = jnp.zeros_like(out_ref)
    for h in range(halves):
        out_ref[h, 0:part, :] = jnp.concatenate(
            [acc_ref[q * part:(q + 1) * part, h * share:(h + 1) * share] for q in range(folds)], axis=1
        )


def local(columns, level_weights, orbit_term, col_owner, col_local, orbit_bin, group_id, departure):
    n_gx, n_gy = lax.axis_size("gx"), lax.axis_size("gy")
    owners = n_gx * n_gy
    nrow = lax.axis_size("row")
    levels, cdev = columns.shape
    npred = level_weights.shape[1]
    nbin = orbit_term.shape[1]
    stripes = LANES // npred
    half = cdev // nrow
    rows = half // stripes
    total = owners * nrow * rows
    if total * LANES * 4 > TABLE_LIMIT or n_gx != 4 or nrow != 2:
        return routed(
            columns, level_weights, orbit_term, col_owner, col_local, orbit_bin, group_id, departure
        )
    footprints = col_local.shape[0]
    nchunks = footprints // CHUNK
    sbits = (stripes - 1).bit_length()
    bbits = (nbin - 1).bit_length()

    mine = lax.dynamic_slice_in_dim(columns, lax.axis_index("row") * half, half, 1)
    vmem = pl.BlockSpec(memory_space=pltpu.VMEM)
    sends = n_gy - 1 + 3 + (n_gy - 1) * 3 + n_gy * 2 + n_gy * 2
    table = pl.pallas_call(
        lambda *refs: table_kernel(*refs, npred=npred, stripes=stripes, n_gy=n_gy, n_row=nrow),
        out_shape=jax.ShapeDtypeStruct((total, LANES), jnp.bfloat16),
        in_specs=[vmem, vmem],
        out_specs=vmem,
        scratch_shapes=[
            pltpu.SemaphoreType.DMA((sends,)),
            pltpu.SemaphoreType.DMA((owners * nrow,)),
        ],
        compiler_params=pltpu.CompilerParams(collective_id=0, has_side_effects=True),
        name="table",
    )(level_weights, mine)

    index = (col_owner[:, 0] * nrow + col_local // half) * rows + col_local % rows
    stripe = (col_local % half) // rows
    packed = stripe | (orbit_bin << sbits) | (group_id << (sbits + bbits))
    orbit = jnp.pad(orbit_term, ((0, 0), (0, LANES - nbin)))
    height = npred * npred + npred + 16
    folds = LANES * nrow // NGRP
    tall = -(-height // (folds * owners * 8)) * owners * 8
    stats = pl.pallas_call(
        lambda *refs: stats_kernel(*refs, npred=npred, stripes=stripes, sbits=sbits, bbits=bbits),
        out_shape=jax.ShapeDtypeStruct((nrow, tall, LANES), jnp.float32),
        in_specs=[pl.BlockSpec(memory_space=pltpu.SMEM), vmem, vmem, vmem, vmem],
        out_specs=vmem,
        scratch_shapes=[
            pltpu.VMEM((total, LANES), jnp.float32),
            pltpu.VMEM((CHUNK, LANES), jnp.float32),
            pltpu.VMEM((CHUNK, LANES), jnp.float32),
            pltpu.VMEM((height, NGRP), jnp.float32),
        ],
        compiler_params=pltpu.CompilerParams(vmem_limit_bytes=40 * 1024 * 1024),
        name="stats",
    )(index, table, packed.reshape(nchunks, CHUNK), departure.reshape(nchunks, CHUNK), orbit)

    share = NGRP // nrow
    devices = owners * nrow
    covariance, cross = pl.pallas_call(
        lambda *refs: reduce_kernel(
            *refs, npred=npred, n_gx=n_gx, n_gy=n_gy, n_row=nrow, height=height
        ),
        out_shape=(
            jax.ShapeDtypeStruct((npred * npred, share), jnp.float32),
            jax.ShapeDtypeStruct((npred, share), jnp.float32),
        ),
        in_specs=[vmem],
        out_specs=(vmem, vmem),
        scratch_shapes=[
            pltpu.VMEM((devices, tall // owners, LANES), jnp.float32),
            pltpu.VMEM((tall, LANES), jnp.float32),
            pltpu.SemaphoreType.DMA((devices - 1,)),
            pltpu.SemaphoreType.DMA((devices,)),
            pltpu.SemaphoreType.DMA((owners - 1,)),
            pltpu.SemaphoreType.DMA((owners,)),
        ],
        compiler_params=pltpu.CompilerParams(collective_id=1, has_side_effects=True),
        name="reduce",
    )(stats)
    return (covariance.reshape(npred, npred, share), cross)


def solution(mesh):
    in_specs = (
        P(None, ("gx", "gy")),
        P(),
        P(),
        P(("gx", "gy", "row"), None),
        P(("gx", "gy", "row")),
        P(("gx", "gy", "row")),
        P(("gx", "gy", "row")),
        P(("gx", "gy", "row")),
    )
    out_specs = (P(None, None, "row"), P(None, "row"))
    return jax.shard_map(local, mesh=mesh, in_specs=in_specs, out_specs=out_specs, check_vma=False)
```

```python
import math

import jax
import jax.numpy as jnp
from jax import lax
from jax.experimental import pallas as pl
from jax.experimental.pallas import tpu as pltpu
from jax.sharding import PartitionSpec as P

NGRP = 64
LANES = 128
CHUNK = 256
TABLE_LIMIT = 24 * 1024 * 1024
AXES = ("gx", "gy", "row")


def send_request(wanted):
    return lax.all_to_all(wanted, ("gx", "gy"), split_axis=0, concat_axis=0, tiled=True)


def send_answer(picked):
    return lax.all_to_all(picked, ("gx", "gy"), split_axis=1, concat_axis=1, tiled=True)


def routed(columns, level_weights, orbit_term, col_owner, col_local, orbit_bin, group_id, departure):
    grid_x = lax.axis_size("gx")
    grid_y = lax.axis_size("gy")
    owners = grid_x * grid_y
    footprints = col_owner.shape[0]
    capacity = 2 * footprints // owners
    slots_all = owners * capacity
    npred = level_weights.shape[1]
    ngroups = NGRP
    owner = col_owner[:, 0]
    owner_hits = (owner[:, None] == jnp.arange(owners, dtype=jnp.int32)[None, :]).astype(jnp.int32)
    ranks = jnp.cumsum(owner_hits, axis=0)
    slot = jnp.sum(ranks * owner_hits, axis=1) - 1
    target = owner * capacity + slot
    stacked = jnp.stack([col_local, orbit_bin, group_id], axis=0)
    placed = jnp.full((3, slots_all), -1, jnp.int32).at[:, target].set(stacked)
    slot_depart = jnp.zeros((slots_all,), jnp.float32).at[target].set(departure)
    wanted = jnp.maximum(placed[0], 0).reshape(owners, capacity)
    asked = send_request(wanted)
    thickness = jnp.dot(level_weights.T, columns, preferred_element_type=jnp.float32).astype(
        jnp.bfloat16
    )
    picked = thickness[:, asked]
    back = send_answer(picked)
    flat = back.reshape(npred, slots_all)
    slot_bin = placed[1]
    slot_group = placed[2]
    width = math.gcd(slots_all, 4096)
    nblocks = slots_all // width
    bin_range = jnp.arange(orbit_term.shape[1], dtype=jnp.int32)
    group_range = jnp.arange(ngroups, dtype=jnp.int32)

    def accumulate(carry, which):
        prod_acc, sum_acc, count_acc = carry
        first = which * width
        part_flat = lax.dynamic_slice_in_dim(flat, first, width, 1)
        part_bin = lax.dynamic_slice_in_dim(slot_bin, first, width, 0)
        grp = lax.dynamic_slice_in_dim(slot_group, first, width, 0)
        dep = lax.dynamic_slice_in_dim(slot_depart, first, width, 0)
        bin_hits = (bin_range[:, None] == part_bin[None, :]).astype(jnp.float32)
        block = part_flat.astype(jnp.float32) + jnp.dot(
            orbit_term,
            bin_hits,
            precision=lax.Precision.HIGHEST,
            preferred_element_type=jnp.float32,
        )
        hits = (grp[:, None] == group_range[None, :]).astype(jnp.float32)
        outer = (block[:, None, :] * block[None, :, :]).reshape(npred * npred, width)
        prod_acc = prod_acc + jnp.dot(
            outer, hits, precision=lax.Precision.HIGHEST, preferred_element_type=jnp.float32
        )
        sum_acc = sum_acc + jnp.dot(
            block * dep[None, :],
            hits,
            precision=lax.Precision.HIGHEST,
            preferred_element_type=jnp.float32,
        )
        count_acc = count_acc + jnp.sum(hits, axis=0)[None, :]
        return ((prod_acc, sum_acc, count_acc), None)

    start = (
        jnp.zeros((npred * npred, ngroups), jnp.float32),
        jnp.zeros((npred, ngroups), jnp.float32),
        jnp.zeros((1, ngroups), jnp.float32),
    )
    (products, sums, count), _ = lax.scan(accumulate, start, jnp.arange(nblocks, dtype=jnp.int32))
    share = ngroups // lax.axis_size("row")
    products, sums, count = (
        lax.psum_scatter(products, "row", scatter_dimension=1, tiled=True),
        lax.psum_scatter(sums, "row", scatter_dimension=1, tiled=True),
        lax.psum_scatter(count, "row", scatter_dimension=1, tiled=True),
    )
    products, sums, count = lax.psum((products, sums, count), ("gx", "gy"))
    scale = 1.0 / (count + 1.0)
    covariance = (products * scale).reshape(npred, npred, share)
    cross = sums * scale
    return (covariance, cross)


def grid_place(gx, gy, row, n_gy, n_row):
    return (gx * n_gy + gy) * n_row + row


def table_kernel(weights_ref, all_columns_ref, out_ref, columns_ref, load_sem, send_sems, recv_sems, *, npred, stripes, n_gy, n_row):
    rows = columns_ref.shape[1] // stripes
    gx, gy, row = lax.axis_index("gx"), lax.axis_index("gy"), lax.axis_index("row")
    low_bit, high_bit = gx % 2, gx // 2
    low_step, high_step = 1 - 2 * low_bit, 2 * (1 - 2 * high_bit)
    gx_a = gx + (1 - row) * low_step + row * high_step
    gx_b = gx + row * low_step + (1 - row) * high_step
    gx_ab = gx + low_step + high_step
    gys = [(gy + i) % n_gy for i in range(n_gy)]
    order = sorted(range(1, n_gy), key=lambda i: min(i, n_gy - i))
    along = [(gx, gys[i], row) for i in order]
    to_a, to_b, mate = (gx_a, gy, row), (gx_b, gy, row), (gx, gy, 1 - row)
    peers = along + [to_a, to_b, mate]

    half = columns_ref.shape[1]
    load = pltpu.make_async_copy(
        all_columns_ref.at[:, pl.ds(pl.multiple_of(row * half, half), half)], columns_ref, load_sem
    )
    load.start()
    barrier = pltpu.get_barrier_semaphore()
    for peer in peers:
        pl.semaphore_signal(barrier, inc=1, device_id=peer, device_id_type=pl.DeviceIdType.MESH)
    load.wait()

    weights = weights_ref[...]
    parts = []
    for s in range(stripes):
        cols = columns_ref[:, s * rows:(s + 1) * rows]
        parts.append(
            lax.dot_general(weights, cols, (((1,), (0,)), ((), ())), preferred_element_type=jnp.float32)
        )
    own = grid_place(gx, gy, row, n_gy, n_row)
    out_ref[pl.ds(pl.multiple_of(own * rows, rows), rows), :] = (
        jnp.concatenate(parts, axis=0).T.astype(jnp.bfloat16)
    )
    pl.semaphore_wait(barrier, len(peers))

    sent = []

    def copy(block, peer, number):
        at = out_ref.at[pl.ds(pl.multiple_of(block * rows, rows), rows), :]
        return pltpu.make_async_remote_copy(
            src_ref=at, dst_ref=at, send_sem=send_sems.at[number], recv_sem=recv_sems.at[block],
            device_id=peer, device_id_type=pl.DeviceIdType.MESH,
        )

    def send(block, targets):
        for peer in targets:
            c = copy(block, peer, len(sent))
            c.start()
            sent.append(c)

    def arrive(block):
        copy(block, mate, 0).wait_recv()

    def place(x, y):
        return grid_place(x, y, row, n_gy, n_row)

    def from_along(i):
        arrive(place(gx, gys[i]))
        send(place(gx, gys[i]), [to_b, to_a, mate])

    def from_a(i):
        arrive(place(gx_a, gys[i]))
        send(place(gx_a, gys[i]), [to_b, mate])

    def from_b(x, i):
        arrive(place(x, gys[i]))
        send(place(x, gys[i]), [mate])

    send(own, [to_a, to_b] + along + [mate])
    from_a(0)
    ahead = []
    for i in order:
        from_along(i)
        if ahead:
            from_a(ahead.pop(0))
        ahead.append(i)
    for i in ahead:
        from_a(i)
    from_b(gx_b, 0)
    from_b(gx_ab, 0)
    for i in order:
        from_b(gx_b, i)
        from_b(gx_ab, i)
    for x in (gx, gx_a, gx_b, gx_ab):
        for y in gys:
            arrive(grid_place(x, y, 1 - row, n_gy, n_row))
    for c in sent:
        c.wait_send()


def reduce_kernel(stats_ref, cov_ref, cross_ref, parts_ref, whole_ref, send_a, recv_a, send_b, recv_b,
                  *, npred, n_gx, n_gy, n_row, height):
    gx, gy, row = lax.axis_index("gx"), lax.axis_index("gy"), lax.axis_index("row")
    owners = n_gx * n_gy
    piece = whole_ref.shape[0] // owners
    mine = gx * n_gy + gy
    others = []
    for dx in range(n_gx):
        for dy in range(n_gy):
            for dr in range(n_row):
                if dx or dy or dr:
                    others.append(((gx + dx) % n_gx, (gy + dy) % n_gy, (row + dr) % n_row))
    barrier = pltpu.get_barrier_semaphore()
    for peer in others:
        pl.semaphore_signal(barrier, inc=1, device_id=peer, device_id_type=pl.DeviceIdType.MESH)
    pl.semaphore_wait(barrier, len(others))

    def rows_of(owner):
        return pl.ds(pl.multiple_of(owner * piece, piece), piece)

    me = mine * n_row + row
    first = []
    for k, peer in enumerate(others):
        owner = peer[0] * n_gy + peer[1]
        c = pltpu.make_async_remote_copy(
            src_ref=stats_ref.at[peer[2], rows_of(owner), :], dst_ref=parts_ref.at[me],
            send_sem=send_a.at[k], recv_sem=recv_a.at[me],
            device_id=peer, device_id_type=pl.DeviceIdType.MESH,
        )
        c.start()
        first.append(c)
    total = stats_ref[row, rows_of(mine), :]
    for k, peer in enumerate(others):
        who = grid_place(peer[0], peer[1], peer[2], n_gy, n_row)
        pltpu.make_async_remote_copy(
            src_ref=stats_ref.at[row, rows_of(mine), :], dst_ref=parts_ref.at[who],
            send_sem=send_a.at[k], recv_sem=recv_a.at[who],
            device_id=peer, device_id_type=pl.DeviceIdType.MESH,
        ).wait_recv()
        total = total + parts_ref[who]
    whole_ref[rows_of(mine), :] = total
    second = []
    for k, peer in enumerate(others):
        if k % n_row == n_row - 1:
            c = pltpu.make_async_remote_copy(
                src_ref=whole_ref.at[rows_of(mine), :], dst_ref=whole_ref.at[rows_of(mine), :],
                send_sem=send_b.at[len(second)], recv_sem=recv_b.at[mine],
                device_id=peer, device_id_type=pl.DeviceIdType.MESH,
            )
            c.start()
            second.append((c, peer))
    for k, (c, peer) in enumerate(second):
        owner = peer[0] * n_gy + peer[1]
        pltpu.make_async_remote_copy(
            src_ref=whole_ref.at[rows_of(owner), :], dst_ref=whole_ref.at[rows_of(owner), :],
            send_sem=send_b.at[k], recv_sem=recv_b.at[owner],
            device_id=peer, device_id_type=pl.DeviceIdType.MESH,
        ).wait_recv()
    share = cov_ref.shape[1]
    folds = LANES // share
    part = height // folds
    flat = jnp.concatenate([whole_ref[0:part, q * share:(q + 1) * share] for q in range(folds)], axis=0)
    square = npred * npred
    scale = 1.0 / (flat[square + npred:square + npred + 1] + 1.0)
    cov_ref[...] = flat[:square] * scale
    cross_ref[...] = flat[square:square + npred] * scale
    for c in first:
        c.wait_send()
    for c, _ in second:
        c.wait_send()


def stats_kernel(index_ref, table_ref, packed_ref, depart_ref, orbit_ref, out_ref, wide_ref, even_ref, odd_ref,
                 acc_ref, *, npred, stripes, sbits, bbits):
    rows = table_ref.shape[0]
    step = 512

    def widen(i, carry):
        at = pl.multiple_of(i * step, step)
        wide_ref[pl.ds(at, step), :] = table_ref[pl.ds(at, step), :].astype(jnp.float32)
        return carry

    lax.fori_loop(0, rows // step, widen, 0)
    nchunks = packed_ref.shape[0]

    def pull(chunk, into):
        names = index_ref.at[pl.ds(chunk * CHUNK, CHUNK)]
        for i in range(CHUNK):
            into[i:i + 1, :] = wide_ref[pl.ds(names[i], 1), :]

    def fold(chunk, held):
        packed = packed_ref[pl.ds(chunk, 1), :]
        dep = depart_ref[pl.ds(chunk, 1), :]
        stripe = packed & (stripes - 1)
        obin = (packed >> sbits) & ((1 << bbits) - 1)
        grp = packed >> (sbits + bbits)
        turned = held[...].T
        stripe = jnp.broadcast_to(stripe, (npred, CHUNK))
        pred = turned[0:npred]
        for s in range(1, stripes):
            pred = jnp.where(stripe == s, turned[s * npred:(s + 1) * npred], pred)
        orbit = orbit_ref[...]
        obin = jnp.broadcast_to(obin, (npred, CHUNK))
        terms = [
            jnp.take_along_axis(orbit, obin[:, a:a + LANES], axis=1, mode="promise_in_bounds")
            for a in range(0, CHUNK, LANES)
        ]
        pred = pred + jnp.concatenate(terms, axis=1)
        hits = (lax.broadcasted_iota(jnp.int32, (NGRP, CHUNK), 0) == grp).astype(jnp.float32).astype(jnp.bfloat16)
        pieces = [pred[i:i + 1, :] * pred for i in range(npred)]
        pieces.append(pred * dep)
        pieces.append(jnp.ones((16, CHUNK), jnp.float32))
        full = jnp.concatenate(pieces, axis=0)
        high = full.astype(jnp.bfloat16)
        low = (full - high.astype(jnp.float32)).astype(jnp.bfloat16)
        dims = (((1,), (1,)), ((), ()))
        return lax.dot_general(high, hits, dims, preferred_element_type=jnp.float32) + lax.dot_general(
            low, hits, dims, preferred_element_type=jnp.float32
        )

    acc_ref[...] = jnp.zeros_like(acc_ref)
    pull(0, even_ref)

    def pair(j, carry):
        pull(2 * j + 1, odd_ref)
        acc_ref[...] += fold(2 * j, even_ref)
        pull(jnp.minimum(2 * j + 2, nchunks - 1), even_ref)
        acc_ref[...] += fold(2 * j + 1, odd_ref)
        return carry

    lax.fori_loop(0, nchunks // 2, pair, 0)
    halves = out_ref.shape[0]
    share = NGRP // halves
    folds = LANES // share
    part = acc_ref.shape[0] // folds
    out_ref[...] = jnp.zeros_like(out_ref)
    for h in range(halves):
        out_ref[h, 0:part, :] = jnp.concatenate(
            [acc_ref[q * part:(q + 1) * part, h * share:(h + 1) * share] for q in range(folds)], axis=1
        )


def local(columns, level_weights, orbit_term, col_owner, col_local, orbit_bin, group_id, departure):
    n_gx, n_gy = lax.axis_size("gx"), lax.axis_size("gy")
    owners = n_gx * n_gy
    nrow = lax.axis_size("row")
    levels, cdev = columns.shape
    npred = level_weights.shape[1]
    nbin = orbit_term.shape[1]
    stripes = LANES // npred
    half = cdev // nrow
    rows = half // stripes
    total = owners * nrow * rows
    if total * LANES * 4 > TABLE_LIMIT or n_gx != 4 or nrow != 2:
        return routed(
            columns, level_weights, orbit_term, col_owner, col_local, orbit_bin, group_id, departure
        )
    footprints = col_local.shape[0]
    nchunks = footprints // CHUNK
    sbits = (stripes - 1).bit_length()
    bbits = (nbin - 1).bit_length()

    vmem = pl.BlockSpec(memory_space=pltpu.VMEM)
    sends = n_gy - 1 + 3 + (n_gy - 1) * 3 + n_gy * 2 + n_gy * 2
    table = pl.pallas_call(
        lambda *refs: table_kernel(*refs, npred=npred, stripes=stripes, n_gy=n_gy, n_row=nrow),
        out_shape=jax.ShapeDtypeStruct((total, LANES), jnp.bfloat16),
        in_specs=[vmem, pl.BlockSpec(memory_space=pl.ANY)],
        out_specs=vmem,
        scratch_shapes=[
            pltpu.VMEM((levels, half), columns.dtype),
            pltpu.SemaphoreType.DMA,
            pltpu.SemaphoreType.DMA((sends,)),
            pltpu.SemaphoreType.DMA((owners * nrow,)),
        ],
        compiler_params=pltpu.CompilerParams(collective_id=0, has_side_effects=True),
        name="table",
    )(level_weights.T, columns)

    index = (col_owner[:, 0] * nrow + col_local // half) * rows + col_local % rows
    stripe = (col_local % half) // rows
    packed = stripe | (orbit_bin << sbits) | (group_id << (sbits + bbits))
    orbit = jnp.pad(orbit_term, ((0, 0), (0, LANES - nbin)))
    height = npred * npred + npred + 16
    folds = LANES * nrow // NGRP
    tall = -(-height // (folds * owners * 8)) * owners * 8
    stats = pl.pallas_call(
        lambda *refs: stats_kernel(*refs, npred=npred, stripes=stripes, sbits=sbits, bbits=bbits),
        out_shape=jax.ShapeDtypeStruct((nrow, tall, LANES), jnp.float32),
        in_specs=[pl.BlockSpec(memory_space=pltpu.SMEM), vmem, vmem, vmem, vmem],
        out_specs=vmem,
        scratch_shapes=[
            pltpu.VMEM((total, LANES), jnp.float32),
            pltpu.VMEM((CHUNK, LANES), jnp.float32),
            pltpu.VMEM((CHUNK, LANES), jnp.float32),
            pltpu.VMEM((height, NGRP), jnp.float32),
        ],
        compiler_params=pltpu.CompilerParams(vmem_limit_bytes=40 * 1024 * 1024),
        name="stats",
    )(index, table, packed.reshape(nchunks, CHUNK), departure.reshape(nchunks, CHUNK), orbit)

    share = NGRP // nrow
    devices = owners * nrow
    covariance, cross = pl.pallas_call(
        lambda *refs: reduce_kernel(
            *refs, npred=npred, n_gx=n_gx, n_gy=n_gy, n_row=nrow, height=height
        ),
        out_shape=(
            jax.ShapeDtypeStruct((npred * npred, share), jnp.float32),
            jax.ShapeDtypeStruct((npred, share), jnp.float32),
        ),
        in_specs=[vmem],
        out_specs=(vmem, vmem),
        scratch_shapes=[
            pltpu.VMEM((devices, tall // owners, LANES), jnp.float32),
            pltpu.VMEM((tall, LANES), jnp.float32),
            pltpu.SemaphoreType.DMA((devices - 1,)),
            pltpu.SemaphoreType.DMA((devices,)),
            pltpu.SemaphoreType.DMA((owners - 1,)),
            pltpu.SemaphoreType.DMA((owners,)),
        ],
        compiler_params=pltpu.CompilerParams(collective_id=1, has_side_effects=True),
        name="reduce",
    )(stats)
    return (covariance.reshape(npred, npred, share), cross)


def solution(mesh):
    in_specs = (
        P(None, ("gx", "gy")),
        P(),
        P(),
        P(("gx", "gy", "row"), None),
        P(("gx", "gy", "row")),
        P(("gx", "gy", "row")),
        P(("gx", "gy", "row")),
        P(("gx", "gy", "row")),
    )
    out_specs = (P(None, None, "row"), P(None, "row"))
    return jax.shard_map(local, mesh=mesh, in_specs=in_specs, out_specs=out_specs, check_vma=False)
```
